128 devices in a mesh: row: 16 (over z, x), col: 8 (over y, core).
Axes of the slice: x: 4, y: 4, z: 4, core: 2. Of those that a mesh axis runs over, the one named last changes fastest.
Arguments:
- embedding: float32 [32768, 128], P(('row', 'col')), may hold values from -6 to 6
- degrees: int32 [32768], P(('row', 'col')), may hold values from 16 to 64
- tile_values: bfloat16 [16, 8, 128, 256, 256], P('row', 'col'), may hold values from -0.1796875 to 0.1796875
- tile_layout: int32 [16, 8, 128, 2], P('row', 'col'), may hold values from 0 to 15, as said below
- tile_count: int32 [16, 8], P('row', 'col'), may hold values from 16 to 128, as said below
- coefficients: float32 [7], replicated, may hold values from -1 to 1
Outputs:
- filtered: float32 [32768, 128], P(('row', 'col'))
The draws below stay inside these ranges and needn't reach their ends.
Inputs may be any that keep to these rules, and one draw needn't show every extreme that they name: `tile_layout`: entry [r, c, s, 0] is a row block below 16 and entry [r, c, s, 1] a column block below 8; entries of slots at or past tile_count[r, c] are valid but unused; a place may repeat. `tile_count`: some device has all 128 slots live.
All inputs are finite; a program needn't handle non-finite values.
Results may differ from the reference program's by a relative error of at most 0.0015.
Values may be sent and summed in bfloat16 or wider, within the bound.
No kernel may reach another device: no remote copies, remote signals or barrier semaphores. Data moves between devices by JAX's collectives and lax.ppermute only.
A program may use at most 128 MiB of HBM per device.

```python
import jax
import jax.numpy as jnp
from jax import lax

F = 128
BLOCK = 256
BLOCKS_DEV = 1
SLOTS = 128
ORDER = 6
PIECE = 256
ROW_BLOCKS = 16
COL_BLOCKS = 8
NODES = 32768
N_ROW = 16
N_COL = 8


def draw_tile_count(key, part):
    key_base = jax.random.fold_in(key, 11)
    key_heavy = jax.random.fold_in(key, 12)
    key_pick = jax.random.fold_in(key, 13)
    key_full = jax.random.fold_in(key, 14)
    lowest = max(1, SLOTS // 8)
    base = jax.random.randint(key_base, (N_ROW * N_COL,), lowest, SLOTS // 2 + 1)
    heavy = jax.random.randint(key_heavy, (N_ROW * N_COL,), SLOTS // 2, SLOTS + 1)
    pick = jax.random.randint(key_pick, (N_ROW * N_COL,), 0, 8)
    counts = jnp.where(pick == 0, heavy, base)
    full_device = jax.random.randint(key_full, (), 0, N_ROW * N_COL)
    counts = jnp.where(jnp.arange(N_ROW * N_COL) == full_device, SLOTS, counts)
    return counts.reshape(N_ROW, N_COL).astype(jnp.int32)


def draw_tile_layout(key, part):
    key_rows = jax.random.fold_in(key, 21)
    key_hub = jax.random.fold_in(key, 22)
    key_pick = jax.random.fold_in(key, 23)
    key_cols = jax.random.fold_in(key, 24)
    rows_any = jax.random.randint(key_rows, (N_ROW, N_COL, SLOTS), 0, ROW_BLOCKS)
    hub_rows = jax.random.randint(key_hub, (N_ROW, N_COL, 1), 0, ROW_BLOCKS)
    pick = jax.random.randint(key_pick, (N_ROW, N_COL, SLOTS), 0, 2)
    rows_all = jnp.where(pick == 1, hub_rows, rows_any)
    cols_all = jax.random.randint(key_cols, (N_ROW, N_COL, SLOTS), 0, COL_BLOCKS)
    return jnp.stack([rows_all, cols_all], axis=-1).astype(jnp.int32)


def touch_ends(drawn, own_key, least, largest):
    place = [jax.random.randint(jax.random.fold_in(own_key, axis), (), 0, length) for axis, length in enumerate(drawn.shape)]
    longest = drawn.shape.index(max(drawn.shape))
    beside = place[:longest] + [(place[longest] + 1) % drawn.shape[longest]] + place[longest + 1:]
    return drawn.at[tuple(place)].set(least).at[tuple(beside)].set(largest)


def shard_levels(rng, shape, pieces, smallest, high):
    loudness, own = 1.0, jax.random.fold_in(rng, 6)
    for axis_at, parts in pieces:
        steps = jnp.exp(jax.random.uniform(jax.random.fold_in(own, axis_at), (parts,), jnp.float32, smallest / len(pieces), high / len(pieces)))
        loudness = loudness * jnp.repeat(steps, shape[axis_at] // parts).reshape([-1 if axis == axis_at else 1 for axis in range(len(shape))])
    return loudness


def normal_values(key, extent, width, limit, pieces=(), held_as=jnp.bfloat16):
    values = jax.random.normal(key, extent, jnp.float32) * width
    if len(pieces) > 0:
        values = shard_levels(key, extent, pieces, -0.22, 0.18) * values
    return jnp.clip(values, min=-limit, max=limit).astype(held_as)


def setup_inputs(seed: int = 0) -> dict:
    seeds = jax.random.split(jax.random.key(seed), 7)
    return {
        "embedding": normal_values(seeds[0], (NODES, F), 1.0, 6.0, ((0, 128),), jnp.float32),
        "degrees": touch_ends(jax.random.randint(seeds[1], (NODES,), 16, 65), jax.random.fold_in(seeds[1], 1), 16, 64).astype(jnp.int32),
        "tile_values": normal_values(seeds[2], (N_ROW, N_COL, SLOTS, BLOCK, BLOCK), 0.03, 0.1796875, ((0, 16), (1, 8))),
        "tile_layout": draw_tile_layout(jax.random.fold_in(seeds[6], 71), 0),
        "tile_count": draw_tile_count(jax.random.fold_in(seeds[6], 71), 0),
        "coefficients": jnp.clip(jax.random.uniform(seeds[5], (ORDER + 1,), jnp.float32, -1.0, 1.0), -1.0, 1.0),
    }


spectral_shift = 0.5

def reference(embedding, degrees, tile_values, tile_layout, tile_count, coefficients):
    inv_root = lax.rsqrt(degrees.astype(jnp.float32))[:, None]

    def operate(vector):
        scaled = (inv_root * vector).astype(jnp.bfloat16)

        def device_step(device_num, running):
            row_group = device_num // N_COL
            col_group = device_num % N_COL
            live_count = tile_count[row_group, col_group]

            def slot_step(slot_num, inner):
                row_block = tile_layout[row_group, col_group, slot_num, 0]
                col_block = tile_layout[row_group, col_group, slot_num, 1]
                col_start = ((row_group * COL_BLOCKS + col_block) * BLOCK).astype(jnp.int32)
                row_start = ((row_block // BLOCKS_DEV * N_COL + col_group) * PIECE + row_block % BLOCKS_DEV * BLOCK).astype(jnp.int32)
                source = lax.dynamic_slice_in_dim(scaled, col_start, BLOCK, 0)
                product = jnp.dot(tile_values[row_group, col_group, slot_num], source, preferred_element_type=jnp.float32)
                before = lax.dynamic_slice_in_dim(inner, row_start, BLOCK, 0)
                return lax.dynamic_update_slice_in_dim(inner, before + product, row_start, 0)
            return lax.fori_loop(jnp.int32(0), live_count, slot_step, running)
        summed = lax.fori_loop(0, N_ROW * N_COL, device_step, jnp.zeros(vector.shape, jnp.float32))
        return (1.0 - spectral_shift) * vector - inv_root * summed
    previous = embedding
    current = operate(embedding)
    filtered = coefficients[0] * previous + coefficients[1] * current
    for order in range(2, ORDER + 1):
        following = 2.0 * operate(current) - previous
        filtered = filtered + coefficients[order] * following
        previous, current = (current, following)
    return filtered
```

```python
import jax
import jax.numpy as jnp
from jax import lax
from jax.experimental import pallas as pl
from jax.experimental.pallas import tpu as pltpu
from jax.sharding import PartitionSpec as P

ORDER = 6

spectral_shift = 0.5
unroll_slots = 8
scale_rows = 16
code_bits = 14
least_largest = 2.0**-100
kernel_vmem = 8 * 1024 * 1024

VMEM = pl.BlockSpec(memory_space=pltpu.VMEM)
SMEM = pl.BlockSpec(memory_space=pltpu.SMEM)


def product_kernel(count_ref, layout_ref, *refs):
    source_refs = refs[:-4]
    tiles_ref, out_ref, stack, total = refs[-4:]
    row_blocks = out_ref.shape[0]
    block_size = total.shape[1]
    live_count = count_ref[0]

    at = 0
    for source_ref in source_refs:
        if len(source_ref.shape) == 3:
            stack[at : at + source_ref.shape[0]] = source_ref[...]
            at += source_ref.shape[0]
        else:
            stack[at] = source_ref[...]
            at += 1
    total[...] = jnp.zeros_like(total)

    def group_step(group, carry):
        for place in range(unroll_slots):
            slot = group * unroll_slots + place
            row_block = jnp.where(slot < live_count, layout_ref[2 * slot], row_blocks)
            col_block = layout_ref[2 * slot + 1]
            total[row_block] += jnp.dot(
                tiles_ref[slot], stack[col_block], preferred_element_type=jnp.float32
            )
        return carry

    lax.fori_loop(0, (live_count + unroll_slots - 1) // unroll_slots, group_step, 0)

    def code_step(row_block, carry):
        values = total[row_block]
        largest = jnp.max(jnp.abs(values), axis=0, keepdims=True)
        power = jnp.ceil(jnp.log2(jnp.maximum(largest, least_largest)))
        codes = jnp.round(values * jnp.exp2(code_bits - power))
        out_ref[row_block, :block_size, :] = codes.astype(jnp.int32).astype(jnp.int16)
        powers = jnp.broadcast_to(power, (scale_rows, power.shape[1]))
        out_ref[row_block, block_size:, :] = powers.astype(jnp.int32).astype(jnp.int16)
        return carry

    lax.fori_loop(0, row_blocks, code_step, 0)


def slot_products(tile_block, layout_flat, live_count, sources, row_blocks):
    block_size = tile_block.shape[1]
    feat_width = sources[0].shape[-1]
    col_blocks = sum(s.shape[0] if s.ndim == 3 else 1 for s in sources)
    return pl.pallas_call(
        product_kernel,
        out_shape=jax.ShapeDtypeStruct(
            (row_blocks, block_size + scale_rows, feat_width), jnp.int16
        ),
        in_specs=[SMEM, SMEM, *[VMEM] * len(sources), VMEM],
        out_specs=VMEM,
        scratch_shapes=[
            pltpu.VMEM((col_blocks, block_size, feat_width), jnp.bfloat16),
            pltpu.VMEM((row_blocks + 1, block_size, feat_width), jnp.float32),
        ],
        compiler_params=pltpu.CompilerParams(vmem_limit_bytes=kernel_vmem),
        name="slot_products",
    )(live_count, layout_flat, *sources, tile_block)


def combine_kernel(first, order, coef_ref, arrived_ref, inv_ref, vector_ref, previous_ref, filtered_ref, *outs):
    block_size = inv_ref.shape[0]
    summed = None
    for peer in range(arrived_ref.shape[0]):
        power = arrived_ref[peer, block_size:, :].astype(jnp.int32).astype(jnp.float32)[:1]
        codes = arrived_ref[peer, :block_size, :].astype(jnp.int32).astype(jnp.float32)
        part = codes * jnp.exp2(power - code_bits)
        summed = part if summed is None else summed + part
    inv_root = inv_ref[...]
    vector = vector_ref[...]
    applied = (1.0 - spectral_shift) * vector - inv_root * summed
    if first:
        following = applied
        filtered = coef_ref[0] * vector + coef_ref[1] * applied
    else:
        following = 2.0 * applied - previous_ref[...]
        filtered = filtered_ref[...] + coef_ref[order] * following
    if len(outs) == 1:
        outs[0][...] = filtered
    else:
        following_out, filtered_out, scaled_out = outs
        following_out[...] = following
        filtered_out[...] = filtered
        scaled_out[...] = (inv_root * following).astype(jnp.bfloat16)


def combine(order, last, coefficients, arrived, inv_root, vector, previous, filtered):
    shape = jax.ShapeDtypeStruct(vector.shape, jnp.float32)
    out_shape = [shape] if last else [shape, shape, jax.ShapeDtypeStruct(vector.shape, jnp.bfloat16)]

    def kernel(*refs):
        combine_kernel(order == 1, order, *refs)

    return pl.pallas_call(
        kernel,
        out_shape=out_shape,
        in_specs=[SMEM, *[VMEM] * 5],
        out_specs=[VMEM] * len(out_shape),
        compiler_params=pltpu.CompilerParams(vmem_limit_bytes=kernel_vmem),
        name="combine",
    )(coefficients, arrived, inv_root, vector, previous, filtered)


def per_device(embedding, degrees, tile_values, tile_layout, tile_count, coefficients):
    tile_block = tile_values[0, 0]
    live_count = tile_count[0]
    row_devices = lax.axis_size("row")
    col_devices = lax.axis_size("col")
    chips = col_devices // 2
    me = lax.axis_index("col")
    layout = tile_layout[0, 0]
    col_block = layout[:, 1]
    col_place = (me // 2 - col_block // 2) % chips + chips * ((me + col_block) % 2)
    layout_flat = jnp.stack([layout[:, 0], col_place], axis=-1).reshape(-1)
    inv_root = jnp.broadcast_to(
        lax.rsqrt(degrees.astype(jnp.float32))[:, None], embedding.shape
    )
    other_core = [(i, i ^ 1) for i in range(col_devices)]

    def gathered(scaled):
        held = [scaled]
        for step in range(1, chips):
            pairs = [(i, (i + 2 * step) % col_devices) for i in range(col_devices)]
            held.append(lax.ppermute(scaled, "col", pairs))
        return held + [lax.ppermute(h, "col", other_core) for h in held]

    scaled = (inv_root * embedding).astype(jnp.bfloat16)
    previous, current, filtered = embedding, embedding, embedding
    for order in range(1, ORDER + 1):
        coded = slot_products(tile_block, layout_flat, live_count, gathered(scaled), row_devices)
        arrived = lax.all_to_all(coded, "row", split_axis=0, concat_axis=0, tiled=True)
        outs = combine(order, order == ORDER, coefficients, arrived, inv_root, current, previous, filtered)
        if order == ORDER:
            return outs[0]
        previous = current
        current, filtered, scaled = outs


def solution(mesh):
    in_specs = (
        P(("row", "col"), None),
        P(("row", "col")),
        P("row", "col", None, None, None),
        P("row", "col", None, None),
        P("row", "col"),
        P(),
    )
    out_specs = P(("row", "col"), None)
    return jax.shard_map(
        per_device, mesh=mesh, in_specs=in_specs, out_specs=out_specs, check_vma=False
    )
```

```python
import functools

import jax
import jax.numpy as jnp
from jax import lax
from jax.experimental import pallas as pl
from jax.experimental.pallas import tpu as pltpu
from jax.sharding import PartitionSpec as P

ORDER = 6

spectral_shift = 0.5
unroll_slots = 16
side = 4
scale_rows = 16
code_bits = 14
least_largest = 2.0**-100
kernel_vmem = 8 * 1024 * 1024

VMEM = pl.BlockSpec(memory_space=pltpu.VMEM)
SMEM = pl.BlockSpec(memory_space=pltpu.SMEM)


def place_in_row():
    row = lax.axis_index("row")
    core = lax.axis_index("col") % 2
    z, x = row // side, row % side
    first = jnp.where(core == 0, x, z)
    second = jnp.where(core == 0, z, x)
    return core, first, second


def block_of(core, first, second):
    return jnp.where(core == 0, second * side + first, first * side + second)


def store_coded(out_ref, at, values):
    block_size = values.shape[0]
    largest = jnp.max(jnp.abs(values), axis=0, keepdims=True)
    power = jnp.ceil(jnp.log2(jnp.maximum(largest, least_largest)))
    codes = jnp.round(values * jnp.exp2(code_bits - power))
    out_ref[at, :block_size, :] = codes.astype(jnp.int32).astype(jnp.int16)
    powers = jnp.broadcast_to(power, (scale_rows, power.shape[1]))
    out_ref[at, block_size:, :] = powers.astype(jnp.int32).astype(jnp.int16)


def decoded(ref, at):
    block_size = ref.shape[1] - scale_rows
    power = ref[at, block_size:, :].astype(jnp.int32).astype(jnp.float32)[:1]
    codes = ref[at, :block_size, :].astype(jnp.int32).astype(jnp.float32)
    return codes * jnp.exp2(power - code_bits)


def product_kernel(count_ref, layout_ref, *refs):
    source_refs = refs[:-7]
    tiles_ref, own_ref, *sent_refs, stack, total = refs[-7:]
    row_blocks = total.shape[0] - 1
    live_count = count_ref[0]

    chips = len(source_refs) // 2
    me = lax.axis_index("col")
    chip, half = me // 2, me % 2
    for step in range(chips):
        from_chip = (chip + chips - step) % chips
        stack[2 * from_chip + half] = source_refs[step][...]
        stack[2 * from_chip + 1 - half] = source_refs[chips + step][...]
    total[...] = jnp.zeros_like(total)

    def group_step(group, carry):
        for place in range(unroll_slots):
            slot = group * unroll_slots + place
            row_block = jnp.where(slot < live_count, layout_ref[0, slot], row_blocks)
            col_block = layout_ref[1, slot]
            total[row_block] += jnp.dot(
                tiles_ref[slot], stack[col_block], preferred_element_type=jnp.float32
            )
        return carry

    lax.fori_loop(0, (live_count + unroll_slots - 1) // unroll_slots, group_step, 0)

    core, first, second = place_in_row()
    for step in range(1, side):

        def code_step(turn, carry):
            block = block_of(core, (first + step) % side, (second + turn) % side)
            store_coded(sent_refs[step - 1], turn, total[block])
            return carry

        lax.fori_loop(0, side, code_step, 0)

    def own_step(turn, carry):
        own_ref[turn] = total[block_of(core, first, (second + turn) % side)]
        return carry

    lax.fori_loop(0, side, own_step, 0)


def slot_products(tile_block, layout, live_count, sources, row_blocks):
    block_size = tile_block.shape[1]
    feat_width = sources[0].shape[-1]
    coded = jax.ShapeDtypeStruct((side, block_size + scale_rows, feat_width), jnp.int16)
    own = jax.ShapeDtypeStruct((side, block_size, feat_width), jnp.float32)
    return pl.pallas_call(
        product_kernel,
        out_shape=[own] + [coded] * (side - 1),
        in_specs=[SMEM, SMEM, *[VMEM] * len(sources), VMEM],
        out_specs=[VMEM] * side,
        scratch_shapes=[
            pltpu.VMEM((len(sources), block_size, feat_width), jnp.bfloat16),
            pltpu.VMEM((row_blocks + 1, block_size, feat_width), jnp.float32),
        ],
        compiler_params=pltpu.CompilerParams(vmem_limit_bytes=kernel_vmem),
        name="slot_products",
    )(live_count, layout, *sources, tile_block)


def middle_kernel(own_ref, *refs):
    arrived_refs, own_out, sent_refs = refs[: side - 1], refs[side - 1], refs[side:]

    def summed(turn):
        value = own_ref[turn]
        for arrived_ref in arrived_refs:
            value = value + decoded(arrived_ref, turn)
        return value

    for turn in range(1, side):
        store_coded(sent_refs[turn - 1], 0, summed(turn))
    own_out[...] = summed(0)


def middle(own, arrived):
    _, block_size, feat_width = own.shape
    coded = jax.ShapeDtypeStruct((1, block_size + scale_rows, feat_width), jnp.int16)
    return pl.pallas_call(
        middle_kernel,
        out_shape=[jax.ShapeDtypeStruct((block_size, feat_width), jnp.float32)]
        + [coded] * (side - 1),
        in_specs=[VMEM] * side,
        out_specs=[VMEM] * side,
        compiler_params=pltpu.CompilerParams(vmem_limit_bytes=kernel_vmem),
        name="middle",
    )(own, *arrived)


def combine_kernel(order, coef_ref, own_ref, *refs):
    arrived_refs = refs[: side - 1]
    inv_ref, vector_ref, previous_ref, filtered_ref, *outs = refs[side - 1 :]
    summed = own_ref[...]
    for arrived_ref in arrived_refs:
        summed = summed + decoded(arrived_ref, 0)
    inv_root = inv_ref[...]
    vector = vector_ref[...]
    applied = (1.0 - spectral_shift) * vector - inv_root * summed
    if order == 1:
        following = applied
        filtered = coef_ref[0] * vector + coef_ref[1] * applied
    else:
        following = 2.0 * applied - previous_ref[...]
        filtered = filtered_ref[...] + coef_ref[order] * following
    if len(outs) == 1:
        outs[0][...] = filtered
    else:
        following_out, filtered_out, scaled_out = outs
        following_out[...] = following
        filtered_out[...] = filtered
        scaled_out[...] = (inv_root * following).astype(jnp.bfloat16)


def combine(order, last, coefficients, own, arrived, inv_root, vector, previous, filtered):
    shape = jax.ShapeDtypeStruct(vector.shape, jnp.float32)
    out_shape = [shape] if last else [shape, shape, jax.ShapeDtypeStruct(vector.shape, jnp.bfloat16)]
    return pl.pallas_call(
        functools.partial(combine_kernel, order),
        out_shape=out_shape,
        in_specs=[SMEM, *[VMEM] * (4 + side)],
        out_specs=[VMEM] * len(out_shape),
        compiler_params=pltpu.CompilerParams(vmem_limit_bytes=kernel_vmem),
        name="combine",
    )(coefficients, own, *arrived, inv_root, vector, previous, filtered)


def pairs_of(rows, cols, target):
    return [
        (row * cols + col, target(row // side, row % side, col // 2, col % 2))
        for row in range(rows)
        for col in range(cols)
    ]


def per_device(embedding, degrees, tile_values, tile_layout, tile_count, coefficients):
    tile_block = tile_values[0, 0]
    live_count = tile_count[0]
    rows = lax.axis_size("row")
    cols = lax.axis_size("col")
    chips = cols // 2
    layout = tile_layout[0, 0].T
    inv_root = jnp.broadcast_to(
        lax.rsqrt(degrees.astype(jnp.float32))[:, None], embedding.shape
    )

    def number(z, x, y, core):
        return (z * side + x) * cols + y * 2 + core

    def send(value, target):
        return lax.ppermute(value, ("row", "col"), pairs_of(rows, cols, target))

    def along_first(value, step):
        def target(z, x, y, core):
            if core == 0:
                return number(z, (x + step) % side, y, core)
            return number((z + step) % side, x, y, core)

        return send(value, target)

    def along_second(value, step):
        def target(z, x, y, core):
            if core == 0:
                return number((z + step) % side, x, y, core)
            return number(z, (x + step) % side, y, core)

        return send(value, target)

    def gathered(scaled):
        held = [scaled]
        for step in range(1, chips):
            held.append(send(scaled, lambda z, x, y, core: number(z, x, (y + step) % chips, core)))
        swapped = [send(h, lambda z, x, y, core: number(z, x, y, 1 - core)) for h in held]
        return held + swapped

    scaled = (inv_root * embedding).astype(jnp.bfloat16)
    previous, current, filtered = embedding, embedding, embedding
    for order in range(1, ORDER + 1):
        own, *sent = slot_products(tile_block, layout, live_count, gathered(scaled), rows)
        arrived = [along_first(part, step) for step, part in enumerate(sent, 1)]
        own, *sent = middle(own, arrived)
        arrived = [along_second(part, step) for step, part in enumerate(sent, 1)]
        outs = combine(
            order, order == ORDER, coefficients, own, arrived, inv_root, current, previous, filtered
        )
        if order == ORDER:
            return outs[0]
        previous = current
        current, filtered, scaled = outs


def solution(mesh):
    in_specs = (
        P(("row", "col"), None),
        P(("row", "col")),
        P("row", "col", None, None, None),
        P("row", "col", None, None),
        P("row", "col"),
        P(),
    )
    out_specs = P(("row", "col"), None)
    return jax.shard_map(
        per_device, mesh=mesh, in_specs=in_specs, out_specs=out_specs, check_vma=False
    )
```

```python
import functools

import jax
import jax.numpy as jnp
from jax import lax
from jax.experimental import pallas as pl
from jax.experimental.pallas import tpu as pltpu
from jax.sharding import PartitionSpec as P

ORDER = 6

spectral_shift = 0.5
slot_mask = 127
col_shift, col_mask = 7, 7
row_shift = 10
side = 4
start_order = (2, 1, 3)
chunk_slots = 8
scale_rows = 16
code_bits = 14
combine_rows = 64
least_largest = 2.0**-100
kernel_vmem = 8 * 1024 * 1024

VMEM = pl.BlockSpec(memory_space=pltpu.VMEM)
SMEM = pl.BlockSpec(memory_space=pltpu.SMEM)


def store_coded(out_ref, at, values):
    block_size = values.shape[0]
    largest = jnp.max(jnp.abs(values), axis=0, keepdims=True)
    power = jnp.ceil(jnp.log2(jnp.maximum(largest, least_largest)))
    codes = jnp.round(values * jnp.exp2(code_bits - power))
    out_ref[at, :block_size, :] = codes.astype(jnp.int32).astype(jnp.int16)
    powers = jnp.broadcast_to(power, (scale_rows, power.shape[1]))
    out_ref[at, block_size:, :] = powers.astype(jnp.int32).astype(jnp.int16)


def decoded(ref, at):
    block_size = ref.shape[1] - scale_rows
    power = ref[at, block_size:, :].astype(jnp.int32).astype(jnp.float32)[:1]
    codes = ref[at, :block_size, :].astype(jnp.int32).astype(jnp.float32)
    return codes * jnp.exp2(power - code_bits)


def load_kernel(count_ref, layout_ref, tiles_ref, held_ref, slots_ref, arrived):
    live_count = count_ref[0]
    live_chunks = (live_count + chunk_slots - 1) // chunk_slots

    def chunk_copy(chunk):
        rows = pl.ds(chunk * chunk_slots, chunk_slots)
        return pltpu.make_async_copy(tiles_ref.at[rows], held_ref.at[rows], arrived.at[chunk])

    def start_chunk(chunk, carry):
        chunk_copy(chunk).start()
        return carry

    lax.fori_loop(0, live_chunks, start_chunk, 0)

    def clear(at, carry):
        for which in range(4):
            slots_ref[which, at] = 0
        return carry

    lax.fori_loop(0, slots_ref.shape[1], clear, 0)

    row = lax.axis_index("row")
    col = lax.axis_index("col")
    chip, core = col // 2, col % 2
    z, x = row // side, row % side
    first = jnp.where(core == 0, x, z)
    second = jnp.where(core == 0, z, x)

    def sort_slot(slot, counts):
        row_block = layout_ref[0, slot]
        col_block = layout_ref[1, slot]
        outer, inner = row_block // side, row_block % side
        step = (jnp.where(core == 0, inner, outer) - first + side) % side
        turn = (jnp.where(core == 0, outer, inner) - second + side) % side
        from_chip = (chip - col_block // 2 + side) % side
        source = from_chip + side * ((col_block + core) % 2)
        stays = step == 0
        near = from_chip == 0
        which = jnp.where(stays, 2, jnp.where(near, 0, 1))
        place = jnp.where(stays, turn, (step - 1) * side + turn)
        at = jnp.where(stays, counts[2], jnp.where(near, counts[0], counts[1]))
        slots_ref[which, at] = slot + (source << col_shift) + (place << row_shift)
        return tuple(n + jnp.where(which == k, 1, 0) for k, n in enumerate(counts))

    counts = lax.fori_loop(0, live_count, sort_slot, (jnp.int32(0), jnp.int32(0), jnp.int32(0)))
    for which in range(3):
        slots_ref[3, which] = counts[which]

    def wait_chunk(chunk, carry):
        chunk_copy(chunk).wait()
        return carry

    lax.fori_loop(0, live_chunks, wait_chunk, 0)


def load_tiles(tile_block, layout, live_count):
    slots = tile_block.shape[0]
    tile_block = pltpu.with_memory_space_constraint(tile_block, pltpu.HBM)
    return pl.pallas_call(
        load_kernel,
        out_shape=[
            pltpu.VMEM(tile_block.shape, tile_block.dtype),
            jax.ShapeDtypeStruct((4, slots), jnp.int32),
        ],
        in_specs=[SMEM, SMEM, pl.BlockSpec(memory_space=pltpu.HBM)],
        out_specs=[VMEM, SMEM],
        scratch_shapes=[pltpu.SemaphoreType.DMA((slots // chunk_slots,))],
        compiler_params=pltpu.CompilerParams(vmem_limit_bytes=kernel_vmem),
        cost_estimate=priced(4000000000),
        name="load_tiles",
    )(live_count, layout, tile_block)


def priced(flops):
    return pl.CostEstimate(flops=flops, bytes_accessed=0, transcendentals=0)


def add_products(which, unroll, slots_ref, tiles_ref, stack, total):
    count = slots_ref[3, which]
    spare = total.shape[0] - 1

    def group_step(group, carry):
        for lane in range(unroll):
            at = group * unroll + lane
            entry = slots_ref[which, at]
            place = jnp.where(at < count, entry >> row_shift, spare)
            total[place] += jnp.dot(
                tiles_ref[entry & slot_mask],
                stack[(entry >> col_shift) & col_mask],
                preferred_element_type=jnp.float32,
            )
        return carry

    lax.fori_loop(0, (count + unroll - 1) // unroll, group_step, 0)


def clear_blocks(ref):
    def clear(at, carry):
        ref[at] = jnp.zeros(ref.shape[1:], ref.dtype)
        return carry

    lax.fori_loop(0, ref.shape[0], clear, 0)


def near_kernel(slots_ref, *refs):
    source_refs, (tiles_ref, total_ref, stack) = refs[:2], refs[2:]
    for at, source_ref in zip((0, side), source_refs):
        stack[at] = source_ref[...]
    clear_blocks(total_ref)
    add_products(0, 4, slots_ref, tiles_ref, stack, total_ref)


def far_kernel(slots_ref, begun_ref, *refs):
    source_refs, (tiles_ref, total_ref, *sent_refs, stack) = refs[:6], refs[6:]
    places = [half * side + step for half in range(2) for step in start_order]
    for at, source_ref in zip(places, source_refs):
        stack[at] = source_ref[...]
    add_products(1, 16, slots_ref, tiles_ref, stack, total_ref)
    for step in range(side - 1):

        def code_step(turn, carry):
            store_coded(sent_refs[step], turn, total_ref[step * side + turn])
            return carry

        lax.fori_loop(0, side, code_step, 0)


def stay_kernel(slots_ref, *refs):
    source_refs, (tiles_ref, own_ref, stack) = refs[:8], refs[8:]
    places = [half * side + step for half in range(2) for step in (0, *start_order)]
    for at, source_ref in zip(places, source_refs):
        stack[at] = source_ref[...]
    clear_blocks(own_ref)
    add_products(2, 4, slots_ref, tiles_ref, stack, own_ref)


def products(held, slots, sources):
    block_size, feat_width = sources[0].shape
    leaving = side * (side - 1)
    total = jax.ShapeDtypeStruct((leaving + 1, block_size, feat_width), jnp.float32)
    stack = pltpu.VMEM((2 * side, block_size, feat_width), jnp.bfloat16)
    coded = jax.ShapeDtypeStruct((side, block_size + scale_rows, feat_width), jnp.int16)
    params = pltpu.CompilerParams(vmem_limit_bytes=kernel_vmem)
    begun = pl.pallas_call(
        near_kernel,
        out_shape=total,
        in_specs=[SMEM, *[VMEM] * 3],
        out_specs=VMEM,
        scratch_shapes=[stack],
        compiler_params=params,
        cost_estimate=priced(1000000000),
        name="near_products",
    )(slots, sources[0], sources[side], held)
    _, *sent = pl.pallas_call(
        far_kernel,
        out_shape=[total] + [coded] * (side - 1),
        in_specs=[SMEM, *[VMEM] * 8],
        out_specs=[VMEM] * side,
        scratch_shapes=[stack],
        input_output_aliases={1: 0},
        compiler_params=params,
        cost_estimate=priced(2000000000),
        name="far_products",
    )(slots, begun, *sources[1:side], *sources[side + 1 :], held)

    def staying():
        return pl.pallas_call(
            stay_kernel,
            out_shape=jax.ShapeDtypeStruct((side + 1, block_size, feat_width), jnp.float32),
            in_specs=[SMEM, *[VMEM] * 9],
            out_specs=VMEM,
            scratch_shapes=[stack],
            compiler_params=params,
            cost_estimate=priced(1000000000),
            name="stay_products",
        )(slots, *sources, held)

    return sent, staying


def middle_kernel(own_ref, *refs):
    arrived_refs, own_out, sent_refs, codes = refs[: side - 1], refs[side - 1], refs[side:-1], refs[-1]

    def summed(turn):
        value = own_ref[turn]
        for arrived_ref in arrived_refs:
            value = value + decoded(arrived_ref, turn)
        return value

    def code_step(step, carry):
        store_coded(codes, step, summed(step + 1))
        return carry

    lax.fori_loop(0, side - 1, code_step, 0)
    for step in range(side - 1):
        sent_refs[step][0] = codes[step]
    own_out[...] = summed(0)


def middle(own, arrived):
    _, block_size, feat_width = own.shape
    coded = jax.ShapeDtypeStruct((1, block_size + scale_rows, feat_width), jnp.int16)
    return pl.pallas_call(
        middle_kernel,
        out_shape=[jax.ShapeDtypeStruct((block_size, feat_width), jnp.float32)]
        + [coded] * (side - 1),
        in_specs=[VMEM] * side,
        out_specs=[VMEM] * side,
        scratch_shapes=[pltpu.VMEM((side - 1, block_size + scale_rows, feat_width), jnp.int16)],
        compiler_params=pltpu.CompilerParams(vmem_limit_bytes=kernel_vmem),
        name="middle",
    )(own, *arrived)


def combine_kernel(order, coef_ref, own_ref, *refs):
    arrived_refs = refs[: side - 1]
    inv_ref, vector_ref, previous_ref, filtered_ref, *outs = refs[side - 1 :]
    block_size = own_ref.shape[0]
    scales = [
        jnp.exp2(ref[0, block_size:, :].astype(jnp.int32).astype(jnp.float32)[:1] - code_bits)
        for ref in arrived_refs
    ]

    def rows_step(part, carry):
        rows = pl.ds(pl.multiple_of(part * combine_rows, combine_rows), combine_rows)
        summed = own_ref[rows, :]
        for ref, scale in zip(arrived_refs, scales):
            summed = summed + ref[0, rows, :].astype(jnp.int32).astype(jnp.float32) * scale
        inv_root = inv_ref[rows, :]
        vector = vector_ref[rows, :]
        applied = (1.0 - spectral_shift) * vector - inv_root * summed
        if order == 1:
            following = applied
            filtered = coef_ref[0] * vector + coef_ref[1] * applied
        else:
            following = 2.0 * applied - previous_ref[rows, :]
            filtered = filtered_ref[rows, :] + coef_ref[order] * following
        if len(outs) == 1:
            outs[0][rows, :] = filtered
        else:
            following_out, filtered_out, scaled_out = outs
            following_out[rows, :] = following
            filtered_out[rows, :] = filtered
            scaled_out[rows, :] = (inv_root * following).astype(jnp.bfloat16)
        return carry

    lax.fori_loop(0, block_size // combine_rows, rows_step, 0)


def combine(order, last, coefficients, own, arrived, inv_root, vector, previous, filtered):
    shape = jax.ShapeDtypeStruct(vector.shape, jnp.float32)
    out_shape = [shape] if last else [shape, shape, jax.ShapeDtypeStruct(vector.shape, jnp.bfloat16)]
    return pl.pallas_call(
        functools.partial(combine_kernel, order),
        out_shape=out_shape,
        in_specs=[SMEM, *[VMEM] * (4 + side)],
        out_specs=[VMEM] * len(out_shape),
        compiler_params=pltpu.CompilerParams(vmem_limit_bytes=kernel_vmem),
        name="combine",
    )(coefficients, own, *arrived, inv_root, vector, previous, filtered)


def pairs_of(rows, cols, target):
    return [
        (row * cols + col, target(row // side, row % side, col // 2, col % 2))
        for row in range(rows)
        for col in range(cols)
    ]


def per_device(embedding, degrees, tile_values, tile_layout, tile_count, coefficients):
    tile_block = tile_values[0, 0]
    live_count = tile_count[0]
    rows = lax.axis_size("row")
    cols = lax.axis_size("col")
    chips = cols // 2
    held, slots = load_tiles(tile_block, tile_layout[0, 0].T, live_count)
    inv_root = jnp.broadcast_to(
        lax.rsqrt(degrees.astype(jnp.float32))[:, None], embedding.shape
    )

    def number(z, x, y, core):
        return (z * side + x) * cols + y * 2 + core

    def send(value, target):
        return lax.ppermute(value, ("row", "col"), pairs_of(rows, cols, target))

    def along_first(value, step):
        def target(z, x, y, core):
            if core == 0:
                return number(z, (x + step) % side, y, core)
            return number((z + step) % side, x, y, core)

        return send(value, target)

    def along_second(value, step):
        def target(z, x, y, core):
            if core == 0:
                return number((z + step) % side, x, y, core)
            return number(z, (x + step) % side, y, core)

        return send(value, target)

    def gathered(scaled):
        held = [scaled]
        for step in start_order:
            held.append(send(scaled, lambda z, x, y, core: number(z, x, (y + step) % chips, core)))
        swapped = [send(h, lambda z, x, y, core: number(z, x, y, 1 - core)) for h in held]
        return held + swapped

    scaled = (inv_root * embedding).astype(jnp.bfloat16)
    previous, current, filtered = embedding, embedding, embedding
    for order in range(1, ORDER + 1):
        sent, staying = products(held, slots, gathered(scaled))
        arrived = [along_first(sent[step - 1], step) for step in start_order]
        own, *sent = middle(staying(), arrived)
        arrived = [along_second(sent[step - 1], step) for step in start_order]
        outs = combine(
            order, order == ORDER, coefficients, own, arrived, inv_root, current, previous, filtered
        )
        if order == ORDER:
            return outs[0]
        previous = current
        current, filtered, scaled = outs


def solution(mesh):
    in_specs = (
        P(("row", "col"), None),
        P(("row", "col")),
        P("row", "col", None, None, None),
        P("row", "col", None, None),
        P("row", "col"),
        P(),
    )
    out_specs = P(("row", "col"), None)
    return jax.shard_map(
        per_device, mesh=mesh, in_specs=in_specs, out_specs=out_specs, check_vma=False
    )
```

```python
import functools

import jax
import jax.numpy as jnp
from jax import lax
from jax.experimental import pallas as pl
from jax.experimental.pallas import tpu as pltpu
from jax.sharding import PartitionSpec as P

ORDER = 6

spectral_shift = 0.5
slot_mask = 127
col_shift, col_mask = 7, 7
row_shift = 10
side = 4
start_order = (2, 1, 3)
chunk_slots = 8
scale_rows = 16
code_bits = 14
combine_rows = 64
least_largest = 2.0**-100
kernel_vmem = 8 * 1024 * 1024

VMEM = pl.BlockSpec(memory_space=pltpu.VMEM)
SMEM = pl.BlockSpec(memory_space=pltpu.SMEM)


def store_coded(out_ref, at, values):
    block_size = values.shape[0]
    largest = jnp.max(jnp.abs(values), axis=0, keepdims=True)
    power = jnp.ceil(jnp.log2(jnp.maximum(largest, least_largest)))
    codes = jnp.round(values * jnp.exp2(code_bits - power))
    out_ref[at, :block_size, :] = codes.astype(jnp.int32).astype(jnp.int16)
    powers = jnp.broadcast_to(power, (scale_rows, power.shape[1]))
    out_ref[at, block_size:, :] = powers.astype(jnp.int32).astype(jnp.int16)


def decoded(ref, at):
    block_size = ref.shape[1] - scale_rows
    power = ref[at, block_size:, :].astype(jnp.int32).astype(jnp.float32)[:1]
    codes = ref[at, :block_size, :].astype(jnp.int32).astype(jnp.float32)
    return codes * jnp.exp2(power - code_bits)


def load_kernel(count_ref, layout_ref, tiles_ref, held_ref, slots_ref, arrived):
    live_count = count_ref[0]
    live_chunks = (live_count + chunk_slots - 1) // chunk_slots

    def chunk_copy(chunk):
        rows = pl.ds(chunk * chunk_slots, chunk_slots)
        return pltpu.make_async_copy(tiles_ref.at[rows], held_ref.at[rows], arrived.at[chunk])

    def start_chunk(chunk, carry):
        chunk_copy(chunk).start()
        return carry

    lax.fori_loop(0, live_chunks, start_chunk, 0)

    def clear(at, carry):
        for which in range(4):
            slots_ref[which, at] = 0
        return carry

    lax.fori_loop(0, slots_ref.shape[1], clear, 0)

    row = lax.axis_index("row")
    col = lax.axis_index("col")
    chip, core = col // 2, col % 2
    z, x = row // side, row % side
    first = jnp.where(core == 0, x, z)
    second = jnp.where(core == 0, z, x)

    def sort_slot(slot, counts):
        row_block = layout_ref[0, slot]
        col_block = layout_ref[1, slot]
        outer, inner = row_block // side, row_block % side
        step = (jnp.where(core == 0, inner, outer) - first + side) % side
        turn = (jnp.where(core == 0, outer, inner) - second + side) % side
        from_chip = (chip - col_block // 2 + side) % side
        source = from_chip + side * ((col_block + core) % 2)
        stays = step == 0
        near = from_chip == 0
        which = jnp.where(stays, 2, jnp.where(near, 0, 1))
        place = jnp.where(stays, turn, (step - 1) * side + turn)
        at = jnp.where(stays, counts[2], jnp.where(near, counts[0], counts[1]))
        slots_ref[which, at] = slot + (source << col_shift) + (place << row_shift)
        return tuple(n + jnp.where(which == k, 1, 0) for k, n in enumerate(counts))

    counts = lax.fori_loop(0, live_count, sort_slot, (jnp.int32(0), jnp.int32(0), jnp.int32(0)))
    for which in range(3):
        slots_ref[3, which] = counts[which]

    def wait_chunk(chunk, carry):
        chunk_copy(chunk).wait()
        return carry

    lax.fori_loop(0, live_chunks, wait_chunk, 0)


def load_tiles(tile_block, layout, live_count):
    slots = tile_block.shape[0]
    tile_block = pltpu.with_memory_space_constraint(tile_block, pltpu.HBM)
    return pl.pallas_call(
        load_kernel,
        out_shape=[
            pltpu.VMEM(tile_block.shape, tile_block.dtype),
            jax.ShapeDtypeStruct((4, slots), jnp.int32),
        ],
        in_specs=[SMEM, SMEM, pl.BlockSpec(memory_space=pltpu.HBM)],
        out_specs=[VMEM, SMEM],
        scratch_shapes=[pltpu.SemaphoreType.DMA((slots // chunk_slots,))],
        compiler_params=pltpu.CompilerParams(vmem_limit_bytes=kernel_vmem),
        cost_estimate=priced(4000000000),
        name="load_tiles",
    )(live_count, layout, tile_block)


def priced(flops):
    return pl.CostEstimate(flops=flops, bytes_accessed=0, transcendentals=0)


def add_products(which, unroll, slots_ref, tiles_ref, stack, total):
    count = slots_ref[3, which]
    spare = total.shape[0] - 1

    def group_step(group, carry):
        for lane in range(unroll):
            at = group * unroll + lane
            entry = slots_ref[which, at]
            place = jnp.where(at < count, entry >> row_shift, spare)
            total[place] += jnp.dot(
                tiles_ref[entry & slot_mask],
                stack[(entry >> col_shift) & col_mask],
                preferred_element_type=jnp.float32,
            )
        return carry

    lax.fori_loop(0, (count + unroll - 1) // unroll, group_step, 0)


def clear_blocks(ref):
    def clear(at, carry):
        ref[at] = jnp.zeros(ref.shape[1:], ref.dtype)
        return carry

    lax.fori_loop(0, ref.shape[0], clear, 0)


def near_kernel(slots_ref, *refs):
    source_refs, (tiles_ref, total_ref, stack) = refs[:2], refs[2:]
    for at, source_ref in zip((0, side), source_refs):
        stack[at] = source_ref[...]
    clear_blocks(total_ref)
    add_products(0, 8, slots_ref, tiles_ref, stack, total_ref)


def put_far(stack, packed_ref, other_ref):
    for at, step in enumerate(start_order):
        stack[step] = packed_ref[at]
        stack[side + step] = other_ref[at]


def far_kernel(slots_ref, begun_ref, packed_ref, other_ref, tiles_ref, total_ref, *refs):
    *sent_refs, stack = refs
    put_far(stack, packed_ref, other_ref)
    add_products(1, 16, slots_ref, tiles_ref, stack, total_ref)
    for step in range(side - 1):

        def code_step(turn, carry):
            store_coded(sent_refs[step], turn, total_ref[step * side + turn])
            return carry

        lax.fori_loop(0, side, code_step, 0)


def stay_kernel(slots_ref, scaled_ref, partner_ref, packed_ref, other_ref, tiles_ref, own_ref, stack):
    stack[0] = scaled_ref[...]
    stack[side] = partner_ref[...]
    put_far(stack, packed_ref, other_ref)
    clear_blocks(own_ref)
    add_products(2, 4, slots_ref, tiles_ref, stack, own_ref)


def pack_kernel(*refs):
    *arrived_refs, packed_ref = refs
    for at, arrived_ref in enumerate(arrived_refs):
        packed_ref[at] = arrived_ref[...]


def pack(arrived):
    first = arrived[0]
    return pl.pallas_call(
        pack_kernel,
        out_shape=jax.ShapeDtypeStruct((len(arrived), *first.shape), first.dtype),
        in_specs=[VMEM] * len(arrived),
        out_specs=VMEM,
        compiler_params=pltpu.CompilerParams(vmem_limit_bytes=kernel_vmem),
        name="pack",
    )(*arrived)


def near_products(held, slots, scaled, partner):
    leaving = side * (side - 1)
    return pl.pallas_call(
        near_kernel,
        out_shape=jax.ShapeDtypeStruct((leaving + 1, *scaled.shape), jnp.float32),
        in_specs=[SMEM, *[VMEM] * 3],
        out_specs=VMEM,
        scratch_shapes=[pltpu.VMEM((2 * side, *scaled.shape), scaled.dtype)],
        compiler_params=pltpu.CompilerParams(vmem_limit_bytes=kernel_vmem),
        cost_estimate=priced(1000000000),
        name="near_products",
    )(slots, scaled, partner, held)


def products(held, slots, begun, sources):
    scaled, partner, packed, other = sources
    block_size, feat_width = scaled.shape
    leaving = side * (side - 1)
    total = jax.ShapeDtypeStruct((leaving + 1, block_size, feat_width), jnp.float32)
    stack = pltpu.VMEM((2 * side, block_size, feat_width), jnp.bfloat16)
    coded = jax.ShapeDtypeStruct((side, block_size + scale_rows, feat_width), jnp.int16)
    params = pltpu.CompilerParams(vmem_limit_bytes=kernel_vmem)
    _, *sent = pl.pallas_call(
        far_kernel,
        out_shape=[total] + [coded] * (side - 1),
        in_specs=[SMEM, *[VMEM] * 4],
        out_specs=[VMEM] * side,
        scratch_shapes=[stack],
        input_output_aliases={1: 0},
        compiler_params=params,
        cost_estimate=priced(2000000000),
        name="far_products",
    )(slots, begun, packed, other, held)

    def staying():
        return pl.pallas_call(
            stay_kernel,
            out_shape=jax.ShapeDtypeStruct((side + 1, block_size, feat_width), jnp.float32),
            in_specs=[SMEM, *[VMEM] * 5],
            out_specs=VMEM,
            scratch_shapes=[stack],
            compiler_params=params,
            cost_estimate=priced(1000000000),
            name="stay_products",
        )(slots, scaled, partner, packed, other, held)

    return sent, staying


def middle_kernel(own_ref, *refs):
    arrived_refs, own_out, sent_refs, codes = refs[: side - 1], refs[side - 1], refs[side:-1], refs[-1]

    def summed(turn):
        value = own_ref[turn]
        for arrived_ref in arrived_refs:
            value = value + decoded(arrived_ref, turn)
        return value

    def code_step(step, carry):
        store_coded(codes, step, summed(step + 1))
        return carry

    lax.fori_loop(0, side - 1, code_step, 0)
    for step in range(side - 1):
        sent_refs[step][0] = codes[step]
    own_out[...] = summed(0)


def middle(own, arrived):
    _, block_size, feat_width = own.shape
    coded = jax.ShapeDtypeStruct((1, block_size + scale_rows, feat_width), jnp.int16)
    return pl.pallas_call(
        middle_kernel,
        out_shape=[jax.ShapeDtypeStruct((block_size, feat_width), jnp.float32)]
        + [coded] * (side - 1),
        in_specs=[VMEM] * side,
        out_specs=[VMEM] * side,
        scratch_shapes=[pltpu.VMEM((side - 1, block_size + scale_rows, feat_width), jnp.int16)],
        compiler_params=pltpu.CompilerParams(vmem_limit_bytes=kernel_vmem),
        name="middle",
    )(own, *arrived)


def combine_kernel(order, coef_ref, own_ref, *refs):
    arrived_refs = refs[: side - 1]
    inv_ref, vector_ref, previous_ref, filtered_ref, *outs = refs[side - 1 :]
    block_size = own_ref.shape[0]
    scales = [
        jnp.exp2(ref[0, block_size:, :].astype(jnp.int32).astype(jnp.float32)[:1] - code_bits)
        for ref in arrived_refs
    ]

    def rows_step(part, carry):
        rows = pl.ds(pl.multiple_of(part * combine_rows, combine_rows), combine_rows)
        summed = own_ref[rows, :]
        for ref, scale in zip(arrived_refs, scales):
            summed = summed + ref[0, rows, :].astype(jnp.int32).astype(jnp.float32) * scale
        inv_root = inv_ref[rows, :]
        vector = vector_ref[rows, :]
        applied = (1.0 - spectral_shift) * vector - inv_root * summed
        if order == 1:
            following = applied
            filtered = coef_ref[0] * vector + coef_ref[1] * applied
        else:
            following = 2.0 * applied - previous_ref[rows, :]
            filtered = filtered_ref[rows, :] + coef_ref[order] * following
        if len(outs) == 1:
            outs[0][rows, :] = filtered
        else:
            following_out, filtered_out, scaled_out = outs
            following_out[rows, :] = following
            filtered_out[rows, :] = filtered
            scaled_out[rows, :] = (inv_root * following).astype(jnp.bfloat16)
        return carry

    lax.fori_loop(0, block_size // combine_rows, rows_step, 0)


def combine(order, last, coefficients, own, arrived, inv_root, vector, previous, filtered):
    shape = jax.ShapeDtypeStruct(vector.shape, jnp.float32)
    out_shape = [shape] if last else [shape, shape, jax.ShapeDtypeStruct(vector.shape, jnp.bfloat16)]
    return pl.pallas_call(
        functools.partial(combine_kernel, order),
        out_shape=out_shape,
        in_specs=[SMEM, *[VMEM] * (4 + side)],
        out_specs=[VMEM] * len(out_shape),
        compiler_params=pltpu.CompilerParams(vmem_limit_bytes=kernel_vmem),
        name="combine",
    )(coefficients, own, *arrived, inv_root, vector, previous, filtered)


def pairs_of(rows, cols, target):
    return [
        (row * cols + col, target(row // side, row % side, col // 2, col % 2))
        for row in range(rows)
        for col in range(cols)
    ]


def per_device(embedding, degrees, tile_values, tile_layout, tile_count, coefficients):
    tile_block = tile_values[0, 0]
    live_count = tile_count[0]
    rows = lax.axis_size("row")
    cols = lax.axis_size("col")
    chips = cols // 2
    held, slots = load_tiles(tile_block, tile_layout[0, 0].T, live_count)
    inv_root = jnp.broadcast_to(
        lax.rsqrt(degrees.astype(jnp.float32))[:, None], embedding.shape
    )

    def number(z, x, y, core):
        return (z * side + x) * cols + y * 2 + core

    def send(value, target):
        return lax.ppermute(value, ("row", "col"), pairs_of(rows, cols, target))

    def along_first(value, step):
        def target(z, x, y, core):
            if core == 0:
                return number(z, (x + step) % side, y, core)
            return number((z + step) % side, x, y, core)

        return send(value, target)

    def along_second(value, step):
        def target(z, x, y, core):
            if core == 0:
                return number((z + step) % side, x, y, core)
            return number(z, (x + step) % side, y, core)

        return send(value, target)

    def gathered(scaled):
        def swap(value):
            return send(value, lambda z, x, y, core: number(z, x, y, 1 - core))

        arrived = [
            send(scaled, lambda z, x, y, core: number(z, x, (y + step) % chips, core))
            for step in start_order
        ]
        partner = swap(scaled)
        begun = near_products(held, slots, scaled, partner)
        begun, *arrived = lax.optimization_barrier((begun, *arrived))
        packed = pack(arrived)
        return begun, (scaled, partner, packed, swap(packed))

    scaled = (inv_root * embedding).astype(jnp.bfloat16)
    previous, current, filtered = embedding, embedding, embedding
    for order in range(1, ORDER + 1):
        begun, sources = gathered(scaled)
        sent, staying = products(held, slots, begun, sources)
        arrived = [along_first(sent[step - 1], step) for step in start_order]
        own, *sent = middle(staying(), arrived)
        arrived = [along_second(sent[step - 1], step) for step in start_order]
        outs = combine(
            order, order == ORDER, coefficients, own, arrived, inv_root, current, previous, filtered
        )
        if order == ORDER:
            return outs[0]
        previous = current
        current, filtered, scaled = outs


def solution(mesh):
    in_specs = (
        P(("row", "col"), None),
        P(("row", "col")),
        P("row", "col", None, None, None),
        P("row", "col", None, None),
        P("row", "col"),
        P(),
    )
    out_specs = P(("row", "col"), None)
    return jax.shard_map(
        per_device, mesh=mesh, in_specs=in_specs, out_specs=out_specs, check_vma=False
    )
```
